32 devices in a mesh: leg: 2 (over y), ping: 8 (over z, core), rng: 2 (over x).
Axes of the slice: x: 2, y: 2, z: 4, core: 2. Of those that a mesh axis runs over, the one named last changes fastest.
Arguments:
- echo: bfloat16 [2, 16384, 256], P(None, ('leg', 'ping'), 'rng'), parts along dimension 1, may hold values from -6 to 6
- steer: bfloat16 [2, 16384, 8192], P(None, ('leg', 'rng'), 'ping'), parts along dimension 1, may hold values from -0.046875 to 0.046875
- offsets: int32 [256], P(('leg', 'ping')), parts along dimension 0, may hold values from 0 to 15
- taps: float32 [256, 4], P(('leg', 'ping')), parts along dimension 0, may hold values from 0.1 to 1
- centers: int32 [512], P(('leg', 'ping', 'rng')), parts along dimension 0, may hold values from 0 to 8191
- halves: int32 [512], P(('leg', 'ping', 'rng')), parts along dimension 0, may hold values from 128 to 1024
Outputs:
- focused: float32 [2, 512, 8192], P(None, ('leg', 'ping', 'rng')), parts along dimension 1
- phase_error: float32 [16384], P('leg'), parts along dimension 0
The draws below stay inside these ranges and needn't reach their ends.
There are 2 independent parts, one for each index of `leg`. The reference program is written for one: setup_inputs(seed, part) draws one part's arguments, and reference() takes and returns one part's arrays. A program takes and returns all parts, laid end to end along the dimension named above; each array names one. Nothing has to cross between parts.
All inputs are finite; a program needn't handle non-finite values.
Results may differ from the reference program's by a relative error of at most 0.0049.
Values may be sent and summed in bfloat16 or wider, within the bound.
A program may use at most 64 MiB of HBM per device.

```python
import math
import jax
import jax.numpy as jnp
from jax import lax

A = 8192
PBLK = 64
NTAP = 4
MAXOFF = 16
R = 256
P_SIZE = 8192
NBLK = 128


def place_ends(array, key, smallest, high):
    place = [jax.random.randint(jax.random.fold_in(key, axis), (), 0, length) for axis, length in enumerate(array.shape)]
    widest = array.shape.index(max(array.shape))
    beside = place[:widest] + [(place[widest] + 1) % array.shape[widest]] + place[widest + 1:]
    return array.at[tuple(place)].set(smallest).at[tuple(beside)].set(high)


def level_of(rng, shape, shards, low, high):
    level, own = 1.0, jax.random.fold_in(rng, 6)
    for axis_at, blocks in shards:
        draws = jnp.exp(jax.random.uniform(jax.random.fold_in(own, axis_at), (blocks,), jnp.float32, low / len(shards), high / len(shards)))
        level = level * jnp.repeat(draws, shape[axis_at] // blocks).reshape([-1 if axis == axis_at else 1 for axis in range(len(shape))])
    return level


def normal_values(key, shape, width, most, pieces=(), kind=jnp.bfloat16):
    entries = width * jax.random.normal(key, shape, jnp.float32)
    if pieces:
        entries = entries * level_of(key, shape, pieces, -0.22, 0.18)
    return jnp.clip(entries, -most, most).astype(kind)


def setup_inputs(seed: int = 0, part: int = 0) -> dict:
    arg_keys = jax.random.split(jax.random.key(seed), 7)
    part_splits = jax.random.split(jax.random.fold_in(arg_keys[6], part), 7)
    return {
        "echo": normal_values(part_splits[0], (2, P_SIZE, R), 1.0, 6.0, ((1, 8), (2, 2))),
        "steer": normal_values(part_splits[1], (2, A, P_SIZE), (2 * P_SIZE) ** -0.5, 0.046875, ((1, 2), (2, 8))),
        "offsets": place_ends(jax.random.randint(part_splits[2], (NBLK,), 0, MAXOFF), jax.random.fold_in(part_splits[2], 1), 0, MAXOFF - 1).astype(jnp.int32),
        "taps": jnp.clip(0.1 + 0.9 * jax.random.uniform(part_splits[3], (NBLK, NTAP), jnp.float32) ** level_of(part_splits[3], (NBLK, NTAP), ((0, 8),), -0.2, 0.2), 0.1, 1.0),
        "centers": place_ends(jax.random.randint(part_splits[4], (R,), 0, A), jax.random.fold_in(part_splits[4], 1), 0, A - 1).astype(jnp.int32),
        "halves": place_ends(jax.random.randint(part_splits[5], (R,), A // 64, A // 8 + 1), jax.random.fold_in(part_splits[5], 1), A // 64, (A // 8 + 1) - 1).astype(jnp.int32),
    }


epsilon = 1e-6


def shift_segment(segment, offset, weights, length):
    margin = MAXOFF + NTAP - 1
    first_col = (margin - offset - (NTAP - 1)).astype(jnp.int32)
    window = lax.dynamic_slice_in_dim(segment, first_col, length + NTAP - 1, axis=2)
    result = jnp.zeros(segment.shape[:2] + (length,), jnp.float32)
    for tap_index in range(NTAP):
        lead_cols = NTAP - 1 - tap_index
        result = result + weights[tap_index] * window[:, :, lead_cols:lead_cols + length]
    return result


def reference(echo, steer, offsets, taps, centers, halves):
    margin = MAXOFF + NTAP - 1
    padded = jnp.pad(echo.astype(jnp.float32), ((0, 0), (0, 0), (margin, 0)))
    blocks = padded.reshape(2, NBLK, PBLK, margin + R)
    shifted = jax.vmap(lambda segment, offset, weights: shift_segment(segment, offset, weights, R),
                       in_axes=(1, 0, 0), out_axes=1)(blocks, offsets, taps)
    interp = shifted.reshape(2, P_SIZE, R).astype(jnp.bfloat16)
    interp = lax.optimization_barrier(interp).astype(jnp.float32)
    weights_full = steer.astype(jnp.float32)
    highest = lax.Precision.HIGHEST
    image_real = jnp.dot(interp[0].T, weights_full[0].T, precision=highest) - jnp.dot(interp[1].T, weights_full[1].T, precision=highest)
    image_imag = jnp.dot(interp[0].T, weights_full[1].T, precision=highest) + jnp.dot(interp[1].T, weights_full[0].T, precision=highest)
    image = lax.complex(image_real, image_imag)
    spectrum = jnp.fft.fft(image, axis=1)
    cells = jnp.arange(A, dtype=jnp.int32)
    distance = (cells[None, :] - centers[:, None]) % A
    distance = jnp.minimum(distance, (A - distance) % A)
    inside = (distance <= halves[:, None]).astype(jnp.float32)
    windowed = jnp.fft.fft(image * inside, axis=1)
    angle = (2.0 * math.pi / A) * centers.astype(jnp.float32)
    turned = lax.complex(jnp.cos(angle), jnp.sin(angle))
    cross = jnp.conj(windowed) * jnp.roll(windowed, -1, axis=1) * turned[:, None]
    numer = jnp.sum(jnp.imag(cross), axis=0)
    denom = jnp.sum(jnp.real(windowed) ** 2 + jnp.imag(windowed) ** 2, axis=0)
    slope = numer / (denom + epsilon)
    phase_error = jnp.cumsum(slope) - slope - jnp.arange(A, dtype=jnp.float32) * (jnp.sum(slope) / A)
    rotation = lax.complex(jnp.cos(phase_error), -jnp.sin(phase_error))
    corrected = jnp.fft.ifft(spectrum * rotation[None, :], axis=1)
    focused = jnp.stack([jnp.real(corrected), jnp.imag(corrected)])
    return focused, phase_error
```

```python
import functools
import math

import jax
import jax.numpy as jnp
from jax import lax
from jax.experimental import pallas as pl
from jax.experimental.pallas import tpu as pltpu
from jax.sharding import PartitionSpec as P

PBLK = 64
NTAP = 4


epsilon = 1e-06


MESH = pl.DeviceIdType.MESH


def meet(peers):
    barrier = pltpu.get_barrier_semaphore()
    for peer in peers:
        pl.semaphore_signal(barrier, inc=1, device_id=peer, device_id_type=MESH)
    pl.semaphore_wait(barrier, len(peers))


def interp_kernel(tiles, offsets_ref, taps_ref, echo_ref, out_ref, held, send_sem, recv_sem, own_sem):
    me = lax.axis_index("rng")
    columns = echo_ref.shape[2]
    width = tiles * columns
    own = pltpu.make_async_copy(echo_ref, held.at[me], own_sem)
    own.start()
    peers = [{"rng": lax.rem(me + step, tiles)} for step in range(1, tiles)]
    meet(peers)
    copies = []
    for step, peer in enumerate(peers):
        copy = pltpu.make_async_remote_copy(
            src_ref=echo_ref,
            dst_ref=held.at[me],
            send_sem=send_sem.at[step],
            recv_sem=recv_sem.at[step],
            device_id=peer,
            device_id_type=MESH,
        )
        copy.start()
        copies.append(copy)
    own.wait()
    for copy in copies:
        copy.wait()

    def block(index, carry):
        rows = pl.ds(pl.multiple_of(index * PBLK, PBLK), PBLK)
        offset = offsets_ref[index]
        for part in range(2):
            value = jnp.concatenate([held[tile, part, rows, :] for tile in range(tiles)], axis=1)
            value = value.astype(jnp.float32)
            column = lax.broadcasted_iota(jnp.int32, (PBLK, width), 1)
            result = jnp.zeros((PBLK, width), jnp.float32)
            for tap in range(NTAP):
                shift = offset + tap
                moved = jnp.where(column >= shift, pltpu.roll(value, shift, axis=1), 0.0)
                result = result + taps_ref[index, tap] * moved
            out_ref[part, rows, :] = result.astype(jnp.bfloat16)
        return carry

    lax.fori_loop(0, out_ref.shape[1] // PBLK, block, 0)


def gather_interp(echo, offsets, taps):
    tiles = lax.axis_size("rng")
    rows, columns = echo.shape[1:]
    vmem = pl.BlockSpec(memory_space=pltpu.VMEM)
    smem = pl.BlockSpec(memory_space=pltpu.SMEM)
    return pl.pallas_call(
        functools.partial(interp_kernel, tiles),
        out_shape=jax.ShapeDtypeStruct((2, rows, tiles * columns), jnp.bfloat16),
        in_specs=[smem, smem, vmem],
        out_specs=vmem,
        scratch_shapes=[
            pltpu.VMEM((tiles, 2, rows, columns), jnp.bfloat16),
            pltpu.SemaphoreType.DMA((tiles - 1,)),
            pltpu.SemaphoreType.DMA((tiles - 1,)),
            pltpu.SemaphoreType.DMA,
        ],
        compiler_params=pltpu.CompilerParams(
            collective_id=0, has_side_effects=True, vmem_limit_bytes=48 * 2**20
        ),
    )(offsets, taps, echo)


def total_kernel(pings, tiles, value_ref, out_ref, held, full, send_sem, recv_sem, send_two, recv_two):
    count = pings * tiles
    me = lax.axis_index("ping") * tiles + lax.axis_index("rng")
    ids = [lax.rem(me + step, count) for step in range(1, count)]
    peers = [{"ping": lax.div(one, tiles), "rng": lax.rem(one, tiles)} for one in ids]
    meet(peers)
    copies = []
    for step, peer in enumerate(peers):
        copy = pltpu.make_async_remote_copy(
            src_ref=value_ref.at[ids[step]],
            dst_ref=held.at[step],
            send_sem=send_sem.at[step],
            recv_sem=recv_sem.at[step],
            device_id=peer,
            device_id_type=MESH,
        )
        copy.start()
        copies.append(copy)
    total = value_ref[me]
    for step, copy in enumerate(copies):
        copy.wait()
        total = total + held[step]
    full[me] = total
    copies = []
    for step, peer in enumerate(peers):
        copy = pltpu.make_async_remote_copy(
            src_ref=full.at[me],
            dst_ref=full.at[me],
            send_sem=send_two.at[step],
            recv_sem=recv_two.at[step],
            device_id=peer,
            device_id_type=MESH,
        )
        copy.start()
        copies.append(copy)
    for copy in copies:
        copy.wait()
    out_ref[...] = full[...]


def total_over(first, second):
    pings, tiles = lax.axis_size("ping"), lax.axis_size("rng")
    count = pings * tiles
    length = first.shape[0]
    value = jnp.concatenate([first, second]).reshape(count, -1, 128)
    vmem = pl.BlockSpec(memory_space=pltpu.VMEM)
    semaphores = pltpu.SemaphoreType.DMA((count - 1,))
    total = pl.pallas_call(
        functools.partial(total_kernel, pings, tiles),
        out_shape=jax.ShapeDtypeStruct(value.shape, jnp.float32),
        in_specs=[vmem],
        out_specs=vmem,
        scratch_shapes=[
            pltpu.VMEM((count - 1,) + value.shape[1:], jnp.float32),
            pltpu.VMEM(value.shape, jnp.float32),
            semaphores,
            semaphores,
            semaphores,
            semaphores,
        ],
        compiler_params=pltpu.CompilerParams(collective_id=1, has_side_effects=True),
    )(value).reshape(2, length)
    return total[0], total[1]


def split_length(length):
    factor_low = 1
    candidate = 1
    while candidate * candidate <= length:
        if length % candidate == 0:
            factor_low = candidate
        candidate = candidate + 1
    return factor_low


def table(rows_count, cols_count, modulus, direction):
    row_ids = jnp.arange(rows_count, dtype=jnp.int32)
    col_ids = jnp.arange(cols_count, dtype=jnp.int32)
    product = row_ids[:, None] * col_ids[None, :] % modulus
    angle = direction * 2.0 * math.pi / modulus * product.astype(jnp.float32)
    return (jnp.cos(angle), jnp.sin(angle))


def transform(real_part, imag_part, direction):
    length = real_part.shape[-1]
    size_low = split_length(length)
    size_high = length // size_low
    lead_shape = real_part.shape[:-1]
    highest = lax.Precision.HIGHEST
    real_grid = real_part.reshape(lead_shape + (size_low, size_high))
    imag_grid = imag_part.reshape(lead_shape + (size_low, size_high))
    first_cos, first_sin = table(size_low, size_low, size_low, direction)
    section_real = jnp.einsum(
        "kn,...nm->...km", first_cos, real_grid, precision=highest
    ) - jnp.einsum("kn,...nm->...km", first_sin, imag_grid, precision=highest)
    section_imag = jnp.einsum(
        "kn,...nm->...km", first_cos, imag_grid, precision=highest
    ) + jnp.einsum("kn,...nm->...km", first_sin, real_grid, precision=highest)
    twist_cos, twist_sin = table(size_low, size_high, length, direction)
    twisted_real = section_real * twist_cos - section_imag * twist_sin
    twisted_imag = section_real * twist_sin + section_imag * twist_cos
    second_cos, second_sin = table(size_high, size_high, size_high, direction)
    final_real = jnp.einsum(
        "bm,...km->...bk", second_cos, twisted_real, precision=highest
    ) - jnp.einsum("bm,...km->...bk", second_sin, twisted_imag, precision=highest)
    final_imag = jnp.einsum(
        "bm,...km->...bk", second_cos, twisted_imag, precision=highest
    ) + jnp.einsum("bm,...km->...bk", second_sin, twisted_real, precision=highest)
    return (final_real.reshape(lead_shape + (length,)), final_imag.reshape(lead_shape + (length,)))


def on_device(echo, steer, offsets, taps, centers, halves):
    echo_piece = gather_interp(echo, offsets, taps)
    part_real = jnp.einsum(
        "pr,ap->ra", echo_piece[0], steer[0], preferred_element_type=jnp.float32
    ) - jnp.einsum("pr,ap->ra", echo_piece[1], steer[1], preferred_element_type=jnp.float32)
    part_imag = jnp.einsum(
        "pr,ap->ra", echo_piece[0], steer[1], preferred_element_type=jnp.float32
    ) + jnp.einsum("pr,ap->ra", echo_piece[1], steer[0], preferred_element_type=jnp.float32)
    partial_value = jnp.stack([part_real, part_imag])
    reduced = lax.psum_scatter(partial_value, "ping", scatter_dimension=1, tiled=True)
    lines_image = lax.all_to_all(reduced, "rng", split_axis=1, concat_axis=2, tiled=True)
    length = lines_image.shape[2]
    cells = jnp.arange(length, dtype=jnp.int32)
    distance = (cells[None, :] - centers[:, None]) % length
    distance = jnp.minimum(distance, (length - distance) % length)
    inside = (distance <= halves[:, None]).astype(jnp.float32)
    stacked_real = jnp.stack([lines_image[0], lines_image[0] * inside])
    stacked_imag = jnp.stack([lines_image[1], lines_image[1] * inside])
    spec_real, spec_imag = transform(stacked_real, stacked_imag, -1.0)
    window_real = spec_real[1]
    window_imag = spec_imag[1]
    next_real = jnp.roll(window_real, -1, axis=1)
    next_imag = jnp.roll(window_imag, -1, axis=1)
    cross_real = window_real * next_real + window_imag * next_imag
    cross_imag = window_real * next_imag - window_imag * next_real
    angle = 2.0 * math.pi / length * centers.astype(jnp.float32)
    numer_local = jnp.sum(
        cross_real * jnp.sin(angle)[:, None] + cross_imag * jnp.cos(angle)[:, None], axis=0
    )
    denom_local = jnp.sum(window_real * window_real + window_imag * window_imag, axis=0)
    numer, denom = total_over(numer_local, denom_local)
    slope = numer / (denom + epsilon)
    phase_error = (
        jnp.cumsum(slope)
        - slope
        - jnp.arange(length, dtype=jnp.float32) * (jnp.sum(slope) / length)
    )
    cos_phase = jnp.cos(phase_error)[None, :]
    sin_phase = jnp.sin(phase_error)[None, :]
    full_real = spec_real[0]
    full_imag = spec_imag[0]
    fixed_real = full_real * cos_phase + full_imag * sin_phase
    fixed_imag = full_imag * cos_phase - full_real * sin_phase
    out_real, out_imag = transform(fixed_real, fixed_imag, 1.0)
    focused = jnp.stack([out_real, out_imag]) / length
    return (focused, phase_error)


def solution(mesh):
    in_specs = (
        P(None, ("leg", "ping"), "rng"),
        P(None, ("leg", "rng"), "ping"),
        P(("leg", "ping")),
        P(("leg", "ping"), None),
        P(("leg", "ping", "rng")),
        P(("leg", "ping", "rng")),
    )
    out_specs = (P(None, ("leg", "ping", "rng"), None), P("leg"))
    return jax.shard_map(
        on_device, mesh=mesh, in_specs=in_specs, out_specs=out_specs, check_vma=False
    )
```
